32 devices in a mesh: gz: 2 (over core), row: 4 (over y, x), col: 4 (over z).
Axes of the slice: x: 2, y: 2, z: 4, core: 2. Of those that a mesh axis runs over, the one named last changes fastest.
Arguments:
- right_sides: float32 [32, 4, 16, 256], P(('gz', 'row', 'col')), may hold values from -6 to 6
- lower_inverse: bfloat16 [32, 4, 256, 256], P(('gz', 'row', 'col')), may hold values from -0.375 to 0.375
- upper_inverse: bfloat16 [32, 4, 256, 256], P(('gz', 'row', 'col')), may hold values from -0.375 to 0.375
- lower_blocks: bfloat16 [32, 4, 2, 256, 256], P(('gz', 'row', 'col')), may hold values from -0.125 to 0.125
- upper_blocks: bfloat16 [32, 4, 2, 256, 256], P(('gz', 'row', 'col')), may hold values from -0.125 to 0.125
- node_widths: int32 [32, 4], P(('gz', 'row', 'col')), may hold values from 128 to 256, as said below
- far_levels: int32 [32, 4], P(('gz', 'row', 'col')), may hold values from 0 to 5, as said below
- owner_level: int32 [32], replicated, may hold values from 0 to 5, as said below
Outputs:
- solution: float32 [32, 4, 16, 256], P(('gz', 'row', 'col'))
The draws below stay inside these ranges and needn't reach their ends.
Inputs may be any that keep to these rules, and one draw needn't show every extreme that they name: Columns c >= node_widths of a supernode are padding; every device holds a supernode with all 256 columns. `far_levels`: between 2 and 5 where the supernode has two or more ancestors, but never past the root; 1 where it has one; 0 for the root and for the slot of the device that owns no separator. `owner_level`: every separator of level u is owned by exactly one device of its group (the devices t with the same t // 2**u); one device owns none and holds 0.
All inputs are finite; a program needn't handle non-finite values.
Results may differ from the reference program's by a relative error of at most 0.018.
Values may be sent and summed in bfloat16 or wider, within the bound.
A program may use at most 64 MiB of HBM per device.

```python
import jax
import jax.numpy as jnp

W = 256
RHS = 16
NB = 2
LOCAL_LEVELS = 2
LOCAL_COUNT = 3
NODES = 4
SUBTREES = 32
UPPER = 5
REACH = 5


def owner_table(key):
    free_ids = jnp.arange(SUBTREES, dtype=jnp.int32)
    owned = jnp.zeros((SUBTREES,), jnp.int32)
    count = SUBTREES
    level = 0
    while count > 1:
        level = level + 1
        pairs = free_ids.reshape(count // 2, 2)
        coin = jax.random.randint(jax.random.fold_in(key, 100 + level), (count // 2,), 0, 2)
        chosen = jnp.where(coin == 1, pairs[:, 1], pairs[:, 0])
        staying = jnp.where(coin == 1, pairs[:, 0], pairs[:, 1])
        owned = owned.at[chosen].set(level)
        free_ids = staying
        count = count // 2
    return owned.astype(jnp.int32)


def draw_owner_level(key, part):
    return owner_table(key)


def draw_node_widths(key, part):
    key_one, key_two = jax.random.split(jax.random.fold_in(key, 23))
    widths = jax.random.randint(key_one, (SUBTREES, NODES), W // 2, W + 1)
    full_slot = jax.random.randint(key_two, (SUBTREES, 1), 0, NODES)
    slots = jnp.arange(NODES, dtype=jnp.int32)[None, :]
    return jnp.where(slots == full_slot, W, widths).astype(jnp.int32)


def draw_far_levels(key, part):
    owners = owner_table(key)
    identities = jnp.arange(SUBTREES, dtype=jnp.int32)
    slots = jnp.arange(NODES, dtype=jnp.int32)
    heights = jnp.zeros((NODES,), jnp.int32)
    for step_at in range(LOCAL_LEVELS):
        heights = jnp.where(slots >= 2 ** LOCAL_LEVELS - 2 ** (LOCAL_LEVELS - step_at), step_at, heights)
    local_room = LOCAL_LEVELS - 1 - heights + UPPER
    owned_room = jnp.where(owners > 0, UPPER - owners, 0)
    room_up = jnp.where(slots[None, :] == NODES - 1, owned_room[:, None], local_room[None, :])
    top_reach = jnp.minimum(room_up, REACH)
    random_bits = jax.random.randint(jax.random.fold_in(key, 31), (SUBTREES, NODES), 0, 1 << 20)
    picked = 2 + random_bits % jnp.maximum(top_reach - 1, 1)
    result = jnp.where(room_up >= 2, picked, room_up).astype(jnp.int32)
    group_owner = []
    for level in range(2, UPPER + 1):
        marked = jnp.where(owners == level, identities, 0)
        summed = marked.reshape(SUBTREES // 2 ** level, 2 ** level).sum(axis=1)
        group_owner.append(jnp.repeat(summed, 2 ** level))
    designated = jnp.zeros((SUBTREES,), jnp.int32)
    for index, level in enumerate(range(2, UPPER + 1)):
        holder = group_owner[index]
        beside = (identities == holder + 1) | (identities == holder - 1)
        designated = jnp.where(beside, level, designated)
    for index, level in enumerate(range(2, UPPER + 1)):
        holder = group_owner[index]
        across = identities == jnp.bitwise_xor(holder, 2 ** (level - 1))
        designated = jnp.where(across, level, designated)
    root_slot = (slots == LOCAL_COUNT - 1)[None, :]
    forced = root_slot & (designated[:, None] > 0)
    return jnp.where(forced, designated[:, None], result).astype(jnp.int32)


def steps_of(key, dims, cuts, smallest, high):
    def one(position, blocks):
        steps = jax.random.uniform(jax.random.fold_in(jax.random.fold_in(key, 6), position), (blocks,), jnp.float32, smallest / len(cuts), high / len(cuts))
        return jnp.repeat(jnp.exp(steps), dims[position] // blocks).reshape((-1,) + (1,) * (len(dims) - position - 1))

    factor_of = one(*cuts[0])
    for cut in cuts[1:]:
        factor_of = factor_of * one(*cut)
    return factor_of


def scatter_about(stream_key, dims, spread, bound, shards=(), kind=jnp.bfloat16):
    loudness = steps_of(stream_key, dims, shards, -0.22, 0.18) if shards else 1.0
    drawn = jax.random.normal(stream_key, dims, jnp.float32) * spread * loudness
    return jnp.minimum(jnp.maximum(drawn, -bound), bound).astype(kind)


def setup_inputs(seed: int = 0) -> dict:
    keys = jax.random.split(jax.random.key(seed), 9)
    return {
        "right_sides": scatter_about(keys[0], (SUBTREES, NODES, RHS, W), 1.0, 6.0, ((0, 32),), jnp.float32),
        "lower_inverse": scatter_about(keys[1], (SUBTREES, NODES, W, W), W ** -0.5, 0.375, ((0, 32),)),
        "upper_inverse": scatter_about(keys[2], (SUBTREES, NODES, W, W), W ** -0.5, 0.375, ((0, 32),)),
        "lower_blocks": scatter_about(keys[3], (SUBTREES, NODES, NB, W, W), (8 * W) ** -0.5, 0.125, ((0, 32),)),
        "upper_blocks": scatter_about(keys[4], (SUBTREES, NODES, NB, W, W), (8 * W) ** -0.5, 0.125, ((0, 32),)),
        "node_widths": draw_node_widths(jax.random.fold_in(keys[8], 71), 0),
        "far_levels": draw_far_levels(jax.random.fold_in(keys[8], 71), 0),
        "owner_level": draw_owner_level(jax.random.fold_in(keys[8], 71), 0),
    }


def level_start(height):
    return 2 ** LOCAL_LEVELS - 2 ** (LOCAL_LEVELS - height)


def apply_blocks(vectors, blocks):
    return jnp.einsum("snrk,snak->snra", vectors.astype(jnp.float32), blocks.astype(jnp.float32))


def apply_single(vectors, blocks):
    return jnp.einsum("srk,sak->sra", vectors.astype(jnp.float32), blocks.astype(jnp.float32))


def forward_local(right_sides, lower_inverse, lower_blocks, padding, far_levels, upper_levels):
    batch_size = right_sides.shape[0]
    pending = jnp.zeros((batch_size, LOCAL_COUNT, RHS, W), jnp.float32)
    upper_pending = jnp.zeros((batch_size, upper_levels, RHS, W), jnp.float32)
    solved = []
    for height in range(LOCAL_LEVELS):
        offset = level_start(height)
        amount = 2 ** (LOCAL_LEVELS - 1 - height)
        residue = (right_sides[:, offset:offset + amount] - pending[:, offset:offset + amount]).astype(jnp.bfloat16)
        solved_now = padding[:, offset:offset + amount] * apply_blocks(residue, lower_inverse[:, offset:offset + amount])
        solved.append(solved_now)
        rounded = solved_now.astype(jnp.bfloat16)
        for block_id in range(NB):
            product = apply_blocks(rounded, lower_blocks[:, offset:offset + amount, block_id])
            for distance in range(1, REACH + 1):
                if block_id == 0 and distance > 1:
                    continue
                if block_id == 0:
                    chosen = product
                else:
                    matches = far_levels[:, offset:offset + amount] == distance
                    chosen = jnp.where(matches[:, :, None, None], product, 0.0)
                target = height + distance
                if target < LOCAL_LEVELS:
                    target_count = amount // 2 ** distance
                    folded = chosen.reshape(batch_size, target_count, 2 ** distance, RHS, W).sum(axis=2)
                    begin_at = level_start(target)
                    pending = pending.at[:, begin_at:begin_at + target_count].add(folded)
                elif target - LOCAL_LEVELS < upper_levels:
                    upper_pending = upper_pending.at[:, target - LOCAL_LEVELS].add(chosen.sum(axis=1))
    return jnp.concatenate(solved, axis=1), upper_pending


def backward_local(forward, upper_inverse, upper_blocks, padding, far_levels, upper_known):
    upper_levels = upper_known.shape[1]
    solutions = [None] * LOCAL_LEVELS
    for height in reversed(range(LOCAL_LEVELS)):
        offset = level_start(height)
        amount = 2 ** (LOCAL_LEVELS - 1 - height)
        residue = forward[:, offset:offset + amount]
        for block_id in range(NB):
            operand = jnp.zeros(residue.shape, jnp.float32)
            for distance in range(1, REACH + 1):
                if block_id == 0 and distance > 1:
                    continue
                target = height + distance
                if target < LOCAL_LEVELS:
                    known_part = jnp.repeat(solutions[target], 2 ** distance, axis=1)
                elif target - LOCAL_LEVELS < upper_levels:
                    known_part = jnp.broadcast_to(upper_known[:, target - LOCAL_LEVELS][:, None], residue.shape)
                else:
                    continue
                if block_id == 0:
                    operand = known_part
                else:
                    matches = far_levels[:, offset:offset + amount] == distance
                    operand = operand + jnp.where(matches[:, :, None, None], known_part, 0.0)
            residue = residue - apply_blocks(operand.astype(jnp.bfloat16), upper_blocks[:, offset:offset + amount, block_id])
        solutions[height] = padding[:, offset:offset + amount] * apply_blocks(residue.astype(jnp.bfloat16), upper_inverse[:, offset:offset + amount])
    return jnp.concatenate(solutions, axis=1)


def reference(right_sides, lower_inverse, upper_inverse, lower_blocks, upper_blocks, node_widths, far_levels, owner_level):
    upper_levels = UPPER
    columns = jnp.arange(W, dtype=jnp.int32)
    padding = (columns[None, None, None, :] < node_widths[:, :, None, None]).astype(jnp.float32)
    forward_nodes, upper_pending = forward_local(
        right_sides[:, :LOCAL_COUNT], lower_inverse[:, :LOCAL_COUNT], lower_blocks[:, :LOCAL_COUNT],
        padding[:, :LOCAL_COUNT], far_levels[:, :LOCAL_COUNT], upper_levels)
    own_rights = right_sides[:, LOCAL_COUNT]
    own_padding = padding[:, LOCAL_COUNT]
    own_far = far_levels[:, LOCAL_COUNT]
    own_forward = jnp.zeros((SUBTREES, RHS, W), jnp.float32)
    for height in range(1, upper_levels + 1):
        group_size = 2 ** height
        totals = upper_pending[:, height - 1].reshape(SUBTREES // group_size, group_size, RHS, W).sum(axis=1)
        gathered = jnp.repeat(totals, group_size, axis=0)
        owner_here = (owner_level == height)[:, None, None]
        residue = (own_rights - gathered).astype(jnp.bfloat16)
        solved_now = jnp.where(owner_here, own_padding * apply_single(residue, lower_inverse[:, LOCAL_COUNT]), 0.0)
        own_forward = own_forward + solved_now
        rounded = solved_now.astype(jnp.bfloat16)
        for block_id in range(NB):
            product = apply_single(rounded, lower_blocks[:, LOCAL_COUNT, block_id])
            for distance in range(1, REACH + 1):
                if block_id == 0 and distance > 1:
                    continue
                target = height + distance
                if target > upper_levels:
                    continue
                if block_id == 0:
                    chosen = product
                else:
                    chosen = jnp.where((own_far == distance)[:, None, None], product, 0.0)
                upper_pending = upper_pending.at[:, target - 1].add(chosen)
    upper_known = jnp.zeros((SUBTREES, upper_levels, RHS, W), jnp.float32)
    own_solution = jnp.zeros((SUBTREES, RHS, W), jnp.float32)
    for height in range(upper_levels, 0, -1):
        group_size = 2 ** height
        owner_here = (owner_level == height)[:, None, None]
        residue = own_forward
        for block_id in range(NB):
            operand = jnp.zeros((SUBTREES, RHS, W), jnp.float32)
            for distance in range(1, REACH + 1):
                if block_id == 0 and distance > 1:
                    continue
                target = height + distance
                if target > upper_levels:
                    continue
                known_part = upper_known[:, target - 1]
                if block_id == 0:
                    operand = known_part
                else:
                    operand = operand + jnp.where((own_far == distance)[:, None, None], known_part, 0.0)
            residue = residue - apply_single(operand.astype(jnp.bfloat16), upper_blocks[:, LOCAL_COUNT, block_id])
        solved_now = jnp.where(owner_here, own_padding * apply_single(residue.astype(jnp.bfloat16), upper_inverse[:, LOCAL_COUNT]), 0.0)
        own_solution = own_solution + solved_now
        totals = solved_now.reshape(SUBTREES // group_size, group_size, RHS, W).sum(axis=1)
        upper_known = upper_known.at[:, height - 1].set(jnp.repeat(totals, group_size, axis=0))
    local_solution = backward_local(
        forward_nodes, upper_inverse[:, :LOCAL_COUNT], upper_blocks[:, :LOCAL_COUNT],
        padding[:, :LOCAL_COUNT], far_levels[:, :LOCAL_COUNT], upper_known)
    return jnp.concatenate([local_solution, own_solution[:, None]], axis=1)
```

```python
import functools

import jax
import jax.numpy as jnp
from jax import lax
from jax.experimental import pallas as pl
from jax.experimental.pallas import tpu as pltpu
from jax.sharding import PartitionSpec as P

W = 256
RHS = 16
NB = 2
LOCAL_LEVELS = 2
LOCAL_COUNT = 3
OWN = LOCAL_COUNT
AXES = ("gz", "row", "col")


def flip_bits(coord, mask):
    flipped = coord
    bit = 1
    while bit <= mask:
        if mask & bit:
            flipped = flipped + bit - 2 * bit * lax.rem(lax.div(coord, bit), 2)
        bit *= 2
    return flipped


def exchange_plan(level, col_levels):
    phases = []
    low = 0
    while low < level:
        high = min(low + 2, col_levels, level) if low < col_levels else min(low + 3, level)
        phases.append([step << low for step in range(1, 1 << (high - low))])
        low = high
    return phases


def times(vectors, matrix):
    return lax.dot_general(
        vectors, matrix, (((1,), (1,)), ((), ())), preferred_element_type=jnp.float32
    )


def half(values):
    return values.astype(jnp.bfloat16)


def kernel(
    spans,
    plans,
    rights_hbm,
    lower_inverse_hbm,
    upper_inverse_hbm,
    lower_blocks_hbm,
    upper_blocks_hbm,
    widths_ref,
    far_ref,
    owner_ref,
    out_ref,
    rights,
    lower_inverse,
    upper_inverse,
    lower_blocks,
    upper_blocks,
    outgoing,
    incoming,
    load_sems,
    send_sems,
    recv_sems,
):
    layer_span, row_span, col_span = spans
    upper_levels = len(plans)
    layer_at = lax.axis_index("gz")
    row_at = lax.axis_index("row")
    col_at = lax.axis_index("col")
    device = (layer_at * row_span + row_at) * col_span + col_at

    def peer(offset):
        return (
            flip_bits(layer_at, offset // (row_span * col_span)),
            flip_bits(row_at, offset // col_span % row_span),
            flip_bits(col_at, offset % col_span),
        )

    pieces = [
        (rights_hbm.at[0], rights),
        (lower_inverse_hbm.at[0, pl.ds(0, 2)], lower_inverse.at[pl.ds(0, 2)]),
        (lower_blocks_hbm.at[0, pl.ds(0, 2)], lower_blocks.at[pl.ds(0, 2)]),
        (lower_inverse_hbm.at[0, pl.ds(2, 2)], lower_inverse.at[pl.ds(2, 2)]),
        (lower_blocks_hbm.at[0, pl.ds(2, 2)], lower_blocks.at[pl.ds(2, 2)]),
        (upper_blocks_hbm.at[0], upper_blocks),
        (upper_inverse_hbm.at[0], upper_inverse),
    ]
    loads = [
        pltpu.make_async_copy(source, target, load_sems.at[at])
        for at, (source, target) in enumerate(pieces)
    ]
    for load in loads:
        load.start()

    barrier = pltpu.get_barrier_semaphore()
    partners = sorted({offset for plan in plans for phase in plan for offset in phase})
    for offset in partners:
        pl.semaphore_signal(
            barrier, inc=1, device_id=peer(offset), device_id_type=pl.DeviceIdType.MESH
        )

    columns = lax.broadcasted_iota(jnp.int32, (RHS, W), 1)

    def padded(slot, values):
        return jnp.where(columns < widths_ref[0, slot], values, 0.0)

    def spread(scalar):
        return jnp.full((RHS, W), scalar, jnp.int32)

    far = [spread(far_ref[0, slot]) for slot in range(LOCAL_COUNT + 1)]
    my_level = spread(owner_ref[device])

    counts = [0, 0]
    sends = []

    def exchange(values, plan, narrow):
        for phase in plan:
            outbox = counts[0]
            counts[0] += 1
            rounded = half(values)
            outgoing[outbox] = rounded
            copies = []
            for offset in phase:
                at = counts[1]
                counts[1] += 1
                copy = pltpu.make_async_remote_copy(
                    src_ref=outgoing.at[outbox],
                    dst_ref=incoming.at[at],
                    send_sem=send_sems.at[at],
                    recv_sem=recv_sems.at[at],
                    device_id=peer(offset),
                    device_id_type=pl.DeviceIdType.MESH,
                )
                copy.start()
                copies.append((copy, at))
            sends.extend(copies)
            if narrow:
                values = rounded.astype(jnp.float32)
            for copy, at in copies:
                copy.wait_recv()
                values = values + incoming[at].astype(jnp.float32)
        return values

    pending = [None] + [jnp.zeros((RHS, W), jnp.float32) for _ in range(upper_levels)]

    def scatter_up(product, slot, height):
        for level in range(1, upper_levels + 1):
            pending[level] = pending[level] + jnp.where(
                far[slot] == level + LOCAL_LEVELS - 1 - height, product, 0.0
            )

    forward = [None] * (LOCAL_COUNT + 1)
    loads[0].wait()
    loads[1].wait()
    for slot in range(2):
        forward[slot] = padded(slot, times(half(rights[slot]), lower_inverse[slot]))
    loads[2].wait()
    near = times(half(forward[0]), lower_blocks[0, 0]) + times(
        half(forward[1]), lower_blocks[1, 0]
    )
    loads[3].wait()
    loads[4].wait()
    forward[2] = padded(2, times(half(rights[2] - near), lower_inverse[2]))
    pending[1] = pending[1] + times(half(forward[2]), lower_blocks[2, 0])
    scatter_up(times(half(forward[2]), lower_blocks[2, 1]), 2, 1)
    for slot in range(2):
        scatter_up(times(half(forward[slot]), lower_blocks[slot, 1]), slot, 0)

    pl.semaphore_wait(barrier, len(partners))

    own_forward = jnp.zeros((RHS, W), jnp.float32)
    for level in range(1, upper_levels + 1):
        gathered = exchange(pending[level], plans[level - 1], False)
        solved = padded(OWN, times(half(rights[OWN] - gathered), lower_inverse[OWN]))
        solved = jnp.where(my_level == level, solved, 0.0)
        own_forward = own_forward + solved
        if level < upper_levels:
            rounded = half(solved)
            pending[level + 1] = pending[level + 1] + times(rounded, lower_blocks[OWN, 0])
            product = times(rounded, lower_blocks[OWN, 1])
            for target in range(level + 1, upper_levels + 1):
                pending[target] = pending[target] + jnp.where(
                    far[OWN] == target - level, product, 0.0
                )

    loads[5].wait()
    loads[6].wait()
    known = [None] * (upper_levels + 1)

    def pick(slot, below):
        chosen = jnp.zeros((RHS, W), jnp.float32)
        for level in range(max(1, below + 1), upper_levels + 1):
            chosen = chosen + jnp.where(far[slot] == level - below, known[level], 0.0)
        return half(chosen)

    own_solution = jnp.zeros((RHS, W), jnp.float32)
    for level in range(upper_levels, 0, -1):
        residue = own_forward
        if level < upper_levels:
            residue = residue - times(half(known[level + 1]), upper_blocks[OWN, 0])
            residue = residue - times(pick(OWN, level), upper_blocks[OWN, 1])
        solved = padded(OWN, times(half(residue), upper_inverse[OWN]))
        solved = jnp.where(my_level == level, solved, 0.0)
        own_solution = own_solution + solved
        known[level] = exchange(solved, plans[level - 1], True)
    out_ref[0, OWN] = own_solution

    residue = forward[2] - times(pick(2, 0), upper_blocks[2, 1])
    residue = residue - times(half(known[1]), upper_blocks[2, 0])
    root = padded(2, times(half(residue), upper_inverse[2]))
    out_ref[0, 2] = root
    for slot in range(2):
        residue = forward[slot] - times(pick(slot, -1), upper_blocks[slot, 1])
        residue = residue - times(half(root), upper_blocks[slot, 0])
        out_ref[0, slot] = padded(slot, times(half(residue), upper_inverse[slot]))

    for copy, _ in sends:
        copy.wait_send()


def local(
    spans,
    right_sides,
    lower_inverse,
    upper_inverse,
    lower_blocks,
    upper_blocks,
    node_widths,
    far_levels,
    owner_level,
):
    layer_span, row_span, col_span = spans
    col_levels = col_span.bit_length() - 1
    upper_levels = (layer_span * row_span * col_span).bit_length() - 1
    plans = [exchange_plan(level, col_levels) for level in range(1, upper_levels + 1)]
    phases = 2 * sum(len(plan) for plan in plans)
    messages = 2 * sum(len(phase) for plan in plans for phase in plan)
    hbm = pl.BlockSpec(memory_space=pl.ANY)
    smem = pl.BlockSpec(memory_space=pltpu.SMEM)
    return pl.pallas_call(
        functools.partial(kernel, spans, plans),
        out_shape=jax.ShapeDtypeStruct(right_sides.shape, jnp.float32),
        in_specs=[hbm] * 5 + [smem] * 3,
        out_specs=pl.BlockSpec(memory_space=pltpu.VMEM),
        scratch_shapes=[
            pltpu.VMEM(right_sides.shape[1:], jnp.float32),
            pltpu.VMEM(lower_inverse.shape[1:], jnp.bfloat16),
            pltpu.VMEM(upper_inverse.shape[1:], jnp.bfloat16),
            pltpu.VMEM(lower_blocks.shape[1:], jnp.bfloat16),
            pltpu.VMEM(upper_blocks.shape[1:], jnp.bfloat16),
            pltpu.VMEM((phases, RHS, W), jnp.bfloat16),
            pltpu.VMEM((messages, RHS, W), jnp.bfloat16),
            pltpu.SemaphoreType.DMA((7,)),
            pltpu.SemaphoreType.DMA((messages,)),
            pltpu.SemaphoreType.DMA((messages,)),
        ],
        compiler_params=pltpu.CompilerParams(collective_id=0, has_side_effects=True),
        name="tree_solve",
    )(
        right_sides,
        lower_inverse,
        upper_inverse,
        lower_blocks,
        upper_blocks,
        node_widths,
        far_levels,
        owner_level,
    )


def solution(mesh):
    spans = tuple(mesh.shape[axis] for axis in AXES)
    split = P(AXES)
    return jax.shard_map(
        functools.partial(local, spans),
        mesh=mesh,
        in_specs=(split,) * 7 + (P(),),
        out_specs=split,
        check_vma=False,
    )
```

```python
import functools

import jax
import jax.numpy as jnp
from jax import lax
from jax.experimental import pallas as pl
from jax.experimental.pallas import tpu as pltpu
from jax.sharding import PartitionSpec as P

W = 256
RHS = 16
NB = 2
LOCAL_LEVELS = 2
LOCAL_COUNT = 3
OWN = LOCAL_COUNT
AXES = ("gz", "row", "col")


def flip_bits(coord, mask):
    flipped = coord
    bit = 1
    while bit <= mask:
        if mask & bit:
            flipped = flipped + bit - 2 * bit * lax.rem(lax.div(coord, bit), 2)
        bit *= 2
    return flipped


def exchange_plan(level, col_levels):
    phases = []
    low = 0
    while low < level:
        high = min(low + 4, level)
        phases.append([step << low for step in range((1 << (high - low)) - 1, 0, -1)])
        low = high
    return phases


def times(vectors, matrix):
    return lax.dot_general(
        vectors, matrix, (((1,), (1,)), ((), ())), preferred_element_type=jnp.float32
    )


def half(values):
    return values.astype(jnp.bfloat16)


def kernel(
    spans,
    plans,
    rights_hbm,
    lower_inverse_hbm,
    upper_inverse_hbm,
    lower_blocks_hbm,
    upper_blocks_hbm,
    widths_ref,
    far_ref,
    owner_ref,
    out_ref,
    rights,
    lower_inverse,
    upper_inverse,
    lower_blocks,
    upper_blocks,
    outgoing,
    incoming,
    fused,
    load_sems,
    send_sems,
    recv_sems,
):
    layer_span, row_span, col_span = spans
    upper_levels = len(plans)
    layer_at = lax.axis_index("gz")
    row_at = lax.axis_index("row")
    col_at = lax.axis_index("col")
    device = (layer_at * row_span + row_at) * col_span + col_at

    def peer(offset):
        return (
            flip_bits(layer_at, offset // (row_span * col_span)),
            flip_bits(row_at, offset // col_span % row_span),
            flip_bits(col_at, offset % col_span),
        )

    pieces = [
        (rights_hbm.at[0], rights),
        (lower_inverse_hbm.at[0, pl.ds(0, 2)], lower_inverse.at[pl.ds(0, 2)]),
        (lower_blocks_hbm.at[0, pl.ds(0, 2)], lower_blocks.at[pl.ds(0, 2)]),
        (lower_inverse_hbm.at[0, pl.ds(2, 2)], lower_inverse.at[pl.ds(2, 2)]),
        (lower_blocks_hbm.at[0, pl.ds(2, 2)], lower_blocks.at[pl.ds(2, 2)]),
        (upper_blocks_hbm.at[0], upper_blocks),
        (upper_inverse_hbm.at[0], upper_inverse),
    ]
    loads = [
        pltpu.make_async_copy(source, target, load_sems.at[at])
        for at, (source, target) in enumerate(pieces)
    ]
    for load in loads:
        load.start()

    barrier = pltpu.get_barrier_semaphore()
    partners = sorted({offset for plan in plans for phase in plan for offset in phase})
    for offset in partners:
        pl.semaphore_signal(
            barrier, inc=1, device_id=peer(offset), device_id_type=pl.DeviceIdType.MESH
        )

    columns = lax.broadcasted_iota(jnp.int32, (RHS, W), 1)

    def spread(scalar):
        return jnp.full((RHS, W), scalar, jnp.int32)

    inside = [columns < widths_ref[0, slot] for slot in range(LOCAL_COUNT + 1)]
    far = [spread(far_ref[0, slot]) for slot in range(LOCAL_COUNT + 1)]
    my_level = spread(owner_ref[device])
    zeros = jnp.zeros((RHS, W), jnp.float32)

    def padded(slot, values):
        return jnp.where(inside[slot], values, 0.0)

    counts = [0, 0]
    sends = []

    def launch(rounded, phase):
        outbox = counts[0]
        counts[0] += 1
        outgoing[outbox] = rounded
        copies = []
        for offset in phase:
            at = counts[1]
            counts[1] += 1
            copy = pltpu.make_async_remote_copy(
                src_ref=outgoing.at[outbox],
                dst_ref=incoming.at[at],
                send_sem=send_sems.at[at],
                recv_sem=recv_sems.at[at],
                device_id=peer(offset),
                device_id_type=pl.DeviceIdType.MESH,
            )
            copy.start()
            copies.append((copy, at))
        sends.extend(copies)
        return copies

    def exchange(values, plan, narrow, beside):
        for index, phase in enumerate(plan):
            rounded = half(values)
            copies = launch(rounded, phase)
            if index == 0:
                beside()
            if narrow:
                values = rounded.astype(jnp.float32)
            for copy, at in copies:
                copy.wait_recv()
                values = values + incoming[at].astype(jnp.float32)
        return values

    pending = [None] + [zeros for _ in range(upper_levels)]

    def scatter_up(product, slot, height):
        for level in range(1, upper_levels + 1):
            pending[level] = pending[level] + jnp.where(
                far[slot] == level + LOCAL_LEVELS - 1 - height, product, 0.0
            )

    forward = [None] * (LOCAL_COUNT + 1)
    loads[0].wait()
    loads[1].wait()
    for slot in range(2):
        forward[slot] = padded(slot, times(half(rights[slot]), lower_inverse[slot]))
    loads[2].wait()
    near = times(half(forward[0]), lower_blocks[0, 0]) + times(
        half(forward[1]), lower_blocks[1, 0]
    )
    for slot in range(2):
        scatter_up(times(half(forward[slot]), lower_blocks[slot, 1]), slot, 0)
    loads[3].wait()
    loads[4].wait()
    forward[2] = padded(2, times(half(rights[2] - near), lower_inverse[2]))
    pending[1] = pending[1] + times(half(forward[2]), lower_blocks[2, 0])
    scatter_up(times(half(forward[2]), lower_blocks[2, 1]), 2, 1)

    pl.semaphore_wait(barrier, len(partners))

    wide_columns = lax.broadcasted_iota(jnp.int32, (W, W), 1)

    def lower_product(block_id):
        kept = jnp.where(
            wide_columns < widths_ref[0, OWN],
            lower_blocks[OWN, block_id].astype(jnp.float32),
            0.0,
        )
        return jnp.dot(half(kept), lower_inverse[OWN], preferred_element_type=jnp.float32)

    def upper_product(slot, block_id):
        return jnp.dot(
            upper_inverse[slot], upper_blocks[slot, block_id], preferred_element_type=jnp.float32
        )

    def split_times(values, matrix):
        large = half(values)
        small = half(values - large.astype(jnp.float32))
        return times(large, matrix) + times(small, matrix)

    far_is_near = jnp.full((W, W), far_ref[0, OWN], jnp.int32) == 1

    own_forward = [zeros]
    residue = [None]

    def own_solve(level):
        solved = padded(OWN, times(residue[0], lower_inverse[OWN]))
        own_forward[0] = own_forward[0] + jnp.where(my_level == level, solved, 0.0)

    def far_up(level):
        product = jnp.where(my_level == level, times(residue[0], fused[1]), 0.0)
        for target in range(level + 2, upper_levels + 1):
            pending[target] = pending[target] + jnp.where(
                far[OWN] == target - level, product, 0.0
            )

    def beside_up(level):
        if level == 1:
            far_product = lower_product(1)
            fused[1] = half(far_product)
            fused[0] = half(lower_product(0) + jnp.where(far_is_near, far_product, 0.0))
        else:
            far_up(level - 1)
            own_solve(level - 1)
        if level == 2:
            loads[5].wait()
            loads[6].wait()
            far_product = upper_product(OWN, 1)
            fused[3] = half(far_product)
            fused[2] = half(upper_product(OWN, 0) + jnp.where(far_is_near, far_product, 0.0))
        if 3 <= level < 3 + LOCAL_COUNT:
            slot = level - 3
            for block_id in range(NB):
                fused[4 + 2 * slot + block_id] = half(upper_product(slot, block_id))

    for level in range(1, upper_levels + 1):
        gathered = exchange(
            pending[level], plans[level - 1], False, functools.partial(beside_up, level)
        )
        residue[0] = half(rights[OWN] - gathered)
        if level < upper_levels:
            product = times(residue[0], fused[0])
            pending[level + 1] = pending[level + 1] + jnp.where(my_level == level, product, 0.0)
    own_solve(upper_levels)

    known = [None] * (upper_levels + 1)

    def pick(slot, below, lowest):
        chosen = zeros
        for level in range(lowest, upper_levels + 1):
            chosen = chosen + jnp.where(far[slot] == level - below, known[level], 0.0)
        return half(chosen)

    base = [split_times(own_forward[0], upper_inverse[OWN])]
    own_solution = zeros
    leaf_base = [None] * LOCAL_COUNT
    far_part = [zeros]

    def beside_down(level):
        if level == upper_levels:
            for slot in range(LOCAL_COUNT):
                leaf_base[slot] = split_times(forward[slot], upper_inverse[slot])
        if 1 < level < upper_levels:
            far_part[0] = times(pick(OWN, level - 1, level + 1), fused[3])
        if level == 1 and upper_levels > 1:
            leaf_base[2] = leaf_base[2] - times(pick(2, 0, 2), fused[4 + 2 * 2 + 1])

    for level in range(upper_levels, 0, -1):
        solved = base[0]
        if level < upper_levels:
            solved = solved - far_part[0] - times(half(known[level + 1]), fused[2])
        solved = jnp.where((my_level == level) & inside[OWN], solved, 0.0)
        own_solution = own_solution + solved
        known[level] = exchange(
            solved, plans[level - 1], True, functools.partial(beside_down, level)
        )
    out_ref[0, OWN] = own_solution

    nearest = half(known[1])
    root = padded(2, leaf_base[2] - times(nearest, fused[4 + 2 * 2]))
    out_ref[0, 2] = root
    for slot in range(2):
        solved = leaf_base[slot] - times(pick(slot, -1, 1), fused[4 + 2 * slot + 1])
        solved = solved - times(half(root), fused[4 + 2 * slot])
        out_ref[0, slot] = padded(slot, solved)

    for copy, _ in sends:
        copy.wait_send()


def local(
    spans,
    right_sides,
    lower_inverse,
    upper_inverse,
    lower_blocks,
    upper_blocks,
    node_widths,
    far_levels,
    owner_level,
):
    layer_span, row_span, col_span = spans
    col_levels = col_span.bit_length() - 1
    upper_levels = (layer_span * row_span * col_span).bit_length() - 1
    plans = [exchange_plan(level, col_levels) for level in range(1, upper_levels + 1)]
    phases = 2 * sum(len(plan) for plan in plans)
    messages = 2 * sum(len(phase) for plan in plans for phase in plan)
    hbm = pl.BlockSpec(memory_space=pl.ANY)
    smem = pl.BlockSpec(memory_space=pltpu.SMEM)
    return pl.pallas_call(
        functools.partial(kernel, spans, plans),
        out_shape=jax.ShapeDtypeStruct(right_sides.shape, jnp.float32),
        in_specs=[hbm] * 5 + [smem] * 3,
        out_specs=pl.BlockSpec(memory_space=pltpu.VMEM),
        scratch_shapes=[
            pltpu.VMEM(right_sides.shape[1:], jnp.float32),
            pltpu.VMEM(lower_inverse.shape[1:], jnp.bfloat16),
            pltpu.VMEM(upper_inverse.shape[1:], jnp.bfloat16),
            pltpu.VMEM(lower_blocks.shape[1:], jnp.bfloat16),
            pltpu.VMEM(upper_blocks.shape[1:], jnp.bfloat16),
            pltpu.VMEM((phases, RHS, W), jnp.bfloat16),
            pltpu.VMEM((messages, RHS, W), jnp.bfloat16),
            pltpu.VMEM((4 + NB * LOCAL_COUNT, W, W), jnp.bfloat16),
            pltpu.SemaphoreType.DMA((7,)),
            pltpu.SemaphoreType.DMA((messages,)),
            pltpu.SemaphoreType.DMA((messages,)),
        ],
        compiler_params=pltpu.CompilerParams(collective_id=0, has_side_effects=True),
        name="tree_solve",
    )(
        right_sides,
        lower_inverse,
        upper_inverse,
        lower_blocks,
        upper_blocks,
        node_widths,
        far_levels,
        owner_level,
    )


def solution(mesh):
    spans = tuple(mesh.shape[axis] for axis in AXES)
    split = P(AXES)
    return jax.shard_map(
        functools.partial(local, spans),
        mesh=mesh,
        in_specs=(split,) * 7 + (P(),),
        out_specs=split,
        check_vma=False,
    )
```

```python
import functools

import jax
import jax.numpy as jnp
from jax import lax
from jax.experimental import pallas as pl
from jax.experimental.pallas import tpu as pltpu
from jax.sharding import PartitionSpec as P

W = 256
RHS = 16
NB = 2
LOCAL_LEVELS = 2
LOCAL_COUNT = 3
OWN = LOCAL_COUNT
AXES = ("gz", "row", "col")


def flip_bits(coord, mask):
    flipped = coord
    bit = 1
    while bit <= mask:
        if mask & bit:
            flipped = flipped + bit - 2 * bit * lax.rem(lax.div(coord, bit), 2)
        bit *= 2
    return flipped


def exchange_plan(level, low=0):
    phases = []
    while low < level:
        high = min(low + 4, level)
        phases.append([step << low for step in range((1 << (high - low)) - 1, 0, -1)])
        low = high
    return phases


def times(vectors, matrix):
    return lax.dot_general(
        vectors, matrix, (((1,), (1,)), ((), ())), preferred_element_type=jnp.float32
    )


def half(values):
    return values.astype(jnp.bfloat16)


HANDOUT = {
    2: ((1, False, 0),),
    3: ((2, False, 0),(1, False, 1)),
    4: ((2, False, 1),(1, True, 0)),
    5: ((1, True, 1),),
}
NEAR_BITS = 2
NEAR = 2**NEAR_BITS


def kernel(
    spans,
    plans,
    down_plans,
    rights_hbm,
    lower_inverse_hbm,
    upper_inverse_hbm,
    lower_blocks_hbm,
    upper_blocks_hbm,
    widths_ref,
    far_ref,
    owner_ref,
    out_ref,
    rights,
    lower_inverse,
    upper_inverse,
    lower_blocks,
    upper_blocks,
    outgoing,
    incoming,
    fused,
    replicas,
    fars,
    bases,
    load_sems,
    send_sems,
    recv_sems,
    bulk_send_sems,
    bulk_recv_sems,
):
    layer_span, row_span, col_span = spans
    upper_levels = len(plans)
    layer_at = lax.axis_index("gz")
    row_at = lax.axis_index("row")
    col_at = lax.axis_index("col")
    device = (layer_at * row_span + row_at) * col_span + col_at

    def peer(offset):
        return (
            flip_bits(layer_at, offset // (row_span * col_span)),
            flip_bits(row_at, offset // col_span % row_span),
            flip_bits(col_at, offset % col_span),
        )

    pieces = [
        (rights_hbm.at[0], rights),
        (lower_inverse_hbm.at[0, pl.ds(0, 2)], lower_inverse.at[pl.ds(0, 2)]),
        (lower_blocks_hbm.at[0, pl.ds(0, 2)], lower_blocks.at[pl.ds(0, 2)]),
        (lower_inverse_hbm.at[0, pl.ds(2, 2)], lower_inverse.at[pl.ds(2, 2)]),
        (lower_blocks_hbm.at[0, pl.ds(2, 2)], lower_blocks.at[pl.ds(2, 2)]),
        (upper_blocks_hbm.at[0], upper_blocks),
        (upper_inverse_hbm.at[0], upper_inverse),
    ]
    loads = [
        pltpu.make_async_copy(source, target, load_sems.at[at])
        for at, (source, target) in enumerate(pieces)
    ]
    for load in loads:
        load.start()

    barrier = pltpu.get_barrier_semaphore()
    partners = sorted({offset for plan in plans for phase in plan for offset in phase})
    for offset in partners:
        pl.semaphore_signal(
            barrier, inc=1, device_id=peer(offset), device_id_type=pl.DeviceIdType.MESH
        )

    columns = lax.broadcasted_iota(jnp.int32, (RHS, W), 1)

    def spread(scalar):
        return jnp.full((RHS, W), scalar, jnp.int32)

    inside = [columns < widths_ref[0, slot] for slot in range(LOCAL_COUNT + 1)]
    far = [spread(far_ref[0, slot]) for slot in range(LOCAL_COUNT + 1)]
    my_level = spread(owner_ref[device])
    zeros = jnp.zeros((RHS, W), jnp.float32)

    def padded(slot, values):
        return jnp.where(inside[slot], values, 0.0)

    counts = [0, 0]
    sends = []

    def launch(rounded, phase):
        outbox = counts[0]
        counts[0] += 1
        outgoing[outbox] = rounded
        copies = []
        for offset in phase:
            at = counts[1]
            counts[1] += 1
            copy = pltpu.make_async_remote_copy(
                src_ref=outgoing.at[outbox],
                dst_ref=incoming.at[at],
                send_sem=send_sems.at[at],
                recv_sem=recv_sems.at[at],
                device_id=peer(offset),
                device_id_type=pl.DeviceIdType.MESH,
            )
            copy.start()
            copies.append((copy, at))
        sends.extend(copies)
        return copies

    bulk = {}

    def hand_out(name, source, target, offset):
        at = len(bulk)
        bulk[name] = pltpu.make_async_remote_copy(
            src_ref=source,
            dst_ref=target,
            send_sem=bulk_send_sems.at[at],
            recv_sem=bulk_recv_sems.at[at],
            device_id=peer(offset),
            device_id_type=pl.DeviceIdType.MESH,
        )
        bulk[name].start()

    received = set()

    def await_bulk(name):
        if name not in received:
            received.add(name)
            bulk[name].wait_recv()

    def exchange(values, plan, narrow, beside):
        for index, phase in enumerate(plan):
            rounded = half(values)
            copies = launch(rounded, phase)
            if index == 0:
                beside()
            if narrow:
                values = rounded.astype(jnp.float32)
            for copy, at in copies:
                copy.wait_recv()
                values = values + incoming[at].astype(jnp.float32)
        return values

    pending = [None] + [zeros for _ in range(upper_levels)]

    def scatter_up(product, slot, height):
        for level in range(1, upper_levels + 1):
            pending[level] = pending[level] + jnp.where(
                far[slot] == level + LOCAL_LEVELS - 1 - height, product, 0.0
            )

    forward = [None] * (LOCAL_COUNT + 1)
    loads[0].wait()
    loads[1].wait()
    for slot in range(2):
        forward[slot] = padded(slot, times(half(rights[slot]), lower_inverse[slot]))
    loads[2].wait()
    near = times(half(forward[0]), lower_blocks[0, 0]) + times(
        half(forward[1]), lower_blocks[1, 0]
    )
    for slot in range(2):
        scatter_up(times(half(forward[slot]), lower_blocks[slot, 1]), slot, 0)
    loads[3].wait()
    loads[4].wait()
    forward[2] = padded(2, times(half(rights[2] - near), lower_inverse[2]))
    pending[1] = pending[1] + times(half(forward[2]), lower_blocks[2, 0])
    scatter_up(times(half(forward[2]), lower_blocks[2, 1]), 2, 1)

    pl.semaphore_wait(barrier, len(partners))

    wide_columns = lax.broadcasted_iota(jnp.int32, (W, W), 1)

    def lower_product(block_id):
        kept = jnp.where(
            wide_columns < widths_ref[0, OWN],
            lower_blocks[OWN, block_id].astype(jnp.float32),
            0.0,
        )
        return jnp.dot(half(kept), lower_inverse[OWN], preferred_element_type=jnp.float32)

    def upper_product(slot, block_id):
        return jnp.dot(
            upper_inverse[slot], upper_blocks[slot, block_id], preferred_element_type=jnp.float32
        )

    def split_times(values, matrix):
        large = half(values)
        small = half(values - large.astype(jnp.float32))
        return times(large, matrix) + times(small, matrix)

    far_is_near = jnp.full((W, W), far_ref[0, OWN], jnp.int32) == 1

    own_forward = [zeros]
    residue = [None]

    def own_solve(level):
        solved = padded(OWN, times(residue[0], lower_inverse[OWN]))
        own_forward[0] = own_forward[0] + jnp.where(my_level == level, solved, 0.0)

    def far_up(level):
        product = jnp.where(my_level == level, times(residue[0], fused[1]), 0.0)
        for target in range(level + 2, upper_levels + 1):
            pending[target] = pending[target] + jnp.where(
                far[OWN] == target - level, product, 0.0
            )

    wide_rows = lax.broadcasted_iota(jnp.int32, (W, W), 0)

    def upper_kept(block_id):
        return jnp.where(
            wide_rows < widths_ref[0, OWN], upper_product(OWN, block_id), 0.0
        )

    def beside_up(level):
        if level == 1:
            fars[0] = far[OWN].astype(jnp.float32)
            for offset in range(1, NEAR):
                hand_out(("far", offset), fars.at[0], fars.at[offset], offset)
            far_product = lower_product(1)
            fused[1] = half(far_product)
            fused[0] = half(lower_product(0) + jnp.where(far_is_near, far_product, 0.0))
            loads[5].wait()
            loads[6].wait()
            far_product = upper_kept(1)
            replicas[0, 1] = half(far_product)
            replicas[0, 0] = half(upper_kept(0) + jnp.where(far_is_near, far_product, 0.0))
        else:
            far_up(level - 1)
            own_solve(level - 1)
        if level == upper_levels:
            bases[0] = padded(OWN, split_times(own_forward[0], upper_inverse[OWN]))
            for offset in reversed(range(1, NEAR)):
                hand_out(("base", offset), bases.at[0], bases.at[offset], offset)
        for offset, relayed, block_id in HANDOUT.get(level, ()):
            kept = 2 if relayed else 0
            if relayed:
                await_bulk((2, False, block_id))
            hand_out(
                (offset, relayed, block_id),
                replicas.at[kept, block_id],
                replicas.at[kept + offset, block_id],
                offset,
            )
        if 3 <= level < 3 + LOCAL_COUNT:
            slot = level - 3
            for block_id in range(NB):
                fused[4 + 2 * slot + block_id] = half(upper_product(slot, block_id))

    for level in range(1, upper_levels + 1):
        gathered = exchange(
            pending[level], plans[level - 1], False, functools.partial(beside_up, level)
        )
        residue[0] = half(rights[OWN] - gathered)
        if level < upper_levels:
            product = times(residue[0], fused[0])
            pending[level + 1] = pending[level + 1] + jnp.where(my_level == level, product, 0.0)
    own_solve(upper_levels)

    known = [None] * (upper_levels + 1)

    def pick(slot, below, lowest):
        chosen = zeros
        for level in range(lowest, upper_levels + 1):
            chosen = chosen + jnp.where(far[slot] == level - below, known[level], 0.0)
        return half(chosen)

    own_solution = zeros
    leaf_base = [None] * LOCAL_COUNT
    far_part = [zeros]
    near_levels = [owner_ref[flip_bits(device, offset)] for offset in range(NEAR)]

    def holder(level):
        offset_of = jnp.int32(0)
        found = jnp.int32(0)
        for offset in range(min(NEAR, 2**level)):
            offset_of = jnp.where(near_levels[offset] == level, offset, offset_of)
            found = jnp.where(near_levels[offset] == level, 1, found)
        return offset_of, found

    def prepare(level):
        if level < 1 or level + 2 > upper_levels:
            return
        at, _ = holder(level)
        reach = fars[at]
        chosen = zeros
        for target in range(level + 2, upper_levels + 1):
            chosen = chosen + jnp.where(reach == float(target - level), known[target], 0.0)
        far_part[0] = times(half(chosen), replicas[at, 1])

    def beside_down(level):
        if level == upper_levels:
            for slot in range(LOCAL_COUNT):
                leaf_base[slot] = split_times(forward[slot], upper_inverse[slot])
        else:
            prepare(level - 1)

    for level in range(upper_levels, 0, -1):
        if level == upper_levels:
            solved = padded(OWN, split_times(own_forward[0], upper_inverse[OWN]))
            solved = jnp.where(my_level == level, solved, 0.0)
        else:
            at, found = holder(level)
            solved = bases[at] - far_part[0] - times(half(known[level + 1]), replicas[at, 0])
            solved = jnp.where(spread(found) == 1, solved, 0.0)
        own_solution = own_solution + jnp.where(my_level == level, solved, 0.0)
        if down_plans[level - 1]:
            known[level] = exchange(
                solved, down_plans[level - 1], True, functools.partial(beside_down, level)
            )
        else:
            known[level] = half(solved).astype(jnp.float32)
            beside_down(level)
        if level == upper_levels:
            for name in bulk:
                await_bulk(name)
    leaf_base[2] = leaf_base[2] - times(pick(2, 0, 2), fused[4 + 2 * 2 + 1])
    out_ref[0, OWN] = own_solution

    nearest = half(known[1])
    root = padded(2, leaf_base[2] - times(nearest, fused[4 + 2 * 2]))
    out_ref[0, 2] = root
    for slot in range(2):
        solved = leaf_base[slot] - times(pick(slot, -1, 1), fused[4 + 2 * slot + 1])
        solved = solved - times(half(root), fused[4 + 2 * slot])
        out_ref[0, slot] = padded(slot, solved)

    for copy, _ in sends:
        copy.wait_send()
    for copy in bulk.values():
        copy.wait_send()


def local(
    spans,
    right_sides,
    lower_inverse,
    upper_inverse,
    lower_blocks,
    upper_blocks,
    node_widths,
    far_levels,
    owner_level,
):
    layer_span, row_span, col_span = spans
    upper_levels = (layer_span * row_span * col_span).bit_length() - 1
    plans = [exchange_plan(level) for level in range(1, upper_levels + 1)]
    down_plans = [exchange_plan(level, NEAR_BITS) for level in range(1, upper_levels)]
    down_plans.append(plans[-1])
    phases = sum(len(plan) for plan in plans + down_plans)
    messages = sum(len(phase) for plan in plans + down_plans for phase in plan)
    handed = 2 * (NEAR - 1) + sum(len(row) for row in HANDOUT.values())
    hbm = pl.BlockSpec(memory_space=pl.ANY)
    smem = pl.BlockSpec(memory_space=pltpu.SMEM)
    return pl.pallas_call(
        functools.partial(kernel, spans, plans, down_plans),
        out_shape=jax.ShapeDtypeStruct(right_sides.shape, jnp.float32),
        in_specs=[hbm] * 5 + [smem] * 3,
        out_specs=pl.BlockSpec(memory_space=pltpu.VMEM),
        scratch_shapes=[
            pltpu.VMEM(right_sides.shape[1:], jnp.float32),
            pltpu.VMEM(lower_inverse.shape[1:], jnp.bfloat16),
            pltpu.VMEM(upper_inverse.shape[1:], jnp.bfloat16),
            pltpu.VMEM(lower_blocks.shape[1:], jnp.bfloat16),
            pltpu.VMEM(upper_blocks.shape[1:], jnp.bfloat16),
            pltpu.VMEM((phases, RHS, W), jnp.bfloat16),
            pltpu.VMEM((messages, RHS, W), jnp.bfloat16),
            pltpu.VMEM((4 + NB * LOCAL_COUNT, W, W), jnp.bfloat16),
            pltpu.VMEM((NEAR, NB, W, W), jnp.bfloat16),
            pltpu.VMEM((NEAR, RHS, W), jnp.float32),
            pltpu.VMEM((NEAR, RHS, W), jnp.float32),
            pltpu.SemaphoreType.DMA((7,)),
            pltpu.SemaphoreType.DMA((messages,)),
            pltpu.SemaphoreType.DMA((messages,)),
            pltpu.SemaphoreType.DMA((handed,)),
            pltpu.SemaphoreType.DMA((handed,)),
        ],
        compiler_params=pltpu.CompilerParams(collective_id=0, has_side_effects=True),
        name="tree_solve",
    )(
        right_sides,
        lower_inverse,
        upper_inverse,
        lower_blocks,
        upper_blocks,
        node_widths,
        far_levels,
        owner_level,
    )


def solution(mesh):
    spans = tuple(mesh.shape[axis] for axis in AXES)
    split = P(AXES)
    return jax.shard_map(
        functools.partial(local, spans),
        mesh=mesh,
        in_specs=(split,) * 7 + (P(),),
        out_specs=split,
        check_vma=False,
    )
```
